128 devices in a mesh: gx: 4 (over y), gy: 4 (over z_hi, core), gz: 8 (over z_lo, x).
Axes of the slice: x: 4, y: 4, z: 4 (z_hi: 2, z_lo: 2; z = z_hi * 2 + z_lo), core: 2. Of those that a mesh axis runs over, the one named last changes fastest.
Arguments:
- volume: bfloat16 [32, 32, 32, 32, 128], P('gx', 'gy', 'gz'), may hold values from -6 to 6
- conv_kernel: bfloat16 [3, 3, 3, 32, 64], replicated, may hold values from -0.21875 to 0.21875
- dense_one: bfloat16 [16, 16, 16, 64, 2048], P('gx', None, None, ('gy', 'gz')), may hold values from -0.01171875 to 0.01171875
- dense_two: float32 [2048, 256], replicated, may hold values from -0.125 to 0.125
- dense_three: float32 [256, 4], replicated, may hold values from -0.375 to 0.375
- targets: float32 [4, 128], replicated, may hold values from -3 to 3
Outputs:
- prediction: float32 [4, 128], replicated
- grad_dense_one: bfloat16 [16, 16, 16, 64, 2048], P('gx', None, None, ('gy', 'gz'))
- grad_conv: float32 [3, 3, 3, 32, 64], replicated
- grad_volume: bfloat16 [32, 32, 32, 32, 128], P('gx', 'gy', 'gz')
The draws below stay inside these ranges and needn't reach their ends.
All inputs are finite; a program needn't handle non-finite values.
Results may differ from the reference program's by a relative error of at most 0.008.
Values may be sent and summed in bfloat16 or wider, within the bound.
No kernel may reach another device: no remote copies, remote signals or barrier semaphores. Data moves between devices by JAX's collectives and lax.ppermute only.
A program may use at most 128 MiB of HBM per device.

```python
import math
import jax
import jax.numpy as jnp
from jax import lax

BATCH = 128
CIN = 32
COUT = 64
HID1 = 2048
HID2 = 256
OUTS = 4
NX = 32
NY = 32
NZ = 32
MX = 16
MY = 16
MZ = 16


def steps_of(rng, shape, pieces, least, top_value):
    def one(position, shards_of):
        draws = jax.random.uniform(jax.random.fold_in(jax.random.fold_in(rng, 6), position), (shards_of,), jnp.float32, least / len(pieces), top_value / len(pieces))
        return jnp.repeat(jnp.exp(draws), shape[position] // shards_of).reshape((-1,) + (1,) * (len(shape) - position - 1))

    factor_of = one(*pieces[0])
    for cut in pieces[1:]:
        factor_of = factor_of * one(*cut)
    return factor_of


def gaussian(key, dims, scale, bound, pieces=(), held_as=jnp.bfloat16):
    values = jax.random.normal(key, dims, jnp.float32) * scale
    if len(pieces) > 0:
        values = steps_of(key, dims, pieces, -0.22, 0.18) * values
    return jnp.clip(values, min=-bound, max=bound).astype(held_as)


def setup_inputs(seed: int = 0) -> dict:
    seeds = jax.random.split(jax.random.key(seed), 7)
    volume = gaussian(seeds[0], (NX, NY, NZ, CIN, BATCH), 1.0, 6.0, ((0, 4), (1, 4), (2, 8)))
    conv_kernel = gaussian(seeds[1], (3, 3, 3, CIN, COUT), (27 * CIN) ** -0.5, 0.21875)
    dense_one = gaussian(seeds[2], (MX, MY, MZ, COUT, HID1), (MX * MY * MZ * COUT) ** -0.5, 0.01171875, ((0, 4), (3, 32)))
    dense_two = gaussian(seeds[3], (HID1, HID2), HID1 ** -0.5, 0.125, (), jnp.float32)
    dense_three = gaussian(seeds[4], (HID2, OUTS), HID2 ** -0.5, 0.375, (), jnp.float32)
    targets = gaussian(seeds[5], (OUTS, BATCH), 0.5, 3.0, (), jnp.float32)
    return {"volume": volume, "conv_kernel": conv_kernel, "dense_one": dense_one, "dense_two": dense_two, "dense_three": dense_three, "targets": targets}


loss_scale = 1024.0
leak_slope = 0.3

def smooth_leaky(values):
    return leak_slope * values + (1.0 - leak_slope) * jax.nn.softplus(values)

def leaky_derivative(values):
    return leak_slope + (1.0 - leak_slope) * jax.nn.sigmoid(values)

def conv_forward(padded, kernel):
    return lax.conv_general_dilated(padded, kernel, (1, 1, 1), 'VALID', dimension_numbers=('DHWCN', 'DHWIO', 'DHWCN'), preferred_element_type=jnp.float32)

def conv_back_input(padded_grad, kernel):
    flipped = kernel[::-1, ::-1, ::-1]
    return lax.conv_general_dilated(padded_grad, flipped, (1, 1, 1), 'VALID', dimension_numbers=('DHWCN', 'DHWOI', 'DHWCN'), preferred_element_type=jnp.float32)

def conv_back_kernel(padded, gradient):
    return lax.conv_general_dilated(padded, gradient, (1, 1, 1), 'VALID', dimension_numbers=('DHWNC', 'DHWOI', 'DHWNC'), preferred_element_type=jnp.float32)

def pooling(values):
    extent_x, extent_y, extent_z, channels, samples = values.shape
    return values.reshape(extent_x // 2, 2, extent_y // 2, 2, extent_z // 2, 2, channels, samples).mean(axis=(1, 3, 5))

def spread(values):
    extent_x, extent_y, extent_z, channels, samples = values.shape
    widened = jnp.broadcast_to(values[:, None, :, None, :, None], (extent_x, 2, extent_y, 2, extent_z, 2, channels, samples))
    return widened.reshape(2 * extent_x, 2 * extent_y, 2 * extent_z, channels, samples)

def split_samples(values, block_count, block_size):
    return jnp.moveaxis(values.reshape(values.shape[:4] + (block_count, block_size)), 4, 0)

def join_samples(values):
    moved = jnp.moveaxis(values, 0, 4)
    return moved.reshape(moved.shape[:4] + (moved.shape[4] * moved.shape[5],))

def reference(volume, conv_kernel, dense_one, dense_two, dense_three, targets):
    samples = volume.shape[4]
    block_size = math.gcd(samples, 16)
    block_count = samples // block_size
    rim = ((1, 1), (1, 1), (1, 1), (0, 0), (0, 0))
    blocks = split_samples(jnp.pad(volume, rim), block_count, block_size)

    def forward_block(padded):
        return pooling(smooth_leaky(conv_forward(padded, conv_kernel))).astype(jnp.bfloat16)
    pooled = join_samples(lax.map(forward_block, blocks))
    features = pooled.reshape(-1, samples)
    weights_flat = dense_one.reshape(-1, dense_one.shape[4])
    pre_one = lax.dot_general(weights_flat, features, (((0,), (0,)), ((), ())), preferred_element_type=jnp.float32)
    hidden_one = smooth_leaky(pre_one)
    pre_two = jnp.dot(dense_two.T, hidden_one, precision=lax.Precision.HIGHEST)
    hidden_two = smooth_leaky(pre_two)
    prediction = jnp.dot(dense_three.T, hidden_two, precision=lax.Precision.HIGHEST)
    error_grad = loss_scale * (prediction - targets)
    grad_pre_two = jnp.dot(dense_three, error_grad, precision=lax.Precision.HIGHEST) * leaky_derivative(pre_two)
    grad_pre_one = (jnp.dot(dense_two, grad_pre_two, precision=lax.Precision.HIGHEST) * leaky_derivative(pre_one)).astype(jnp.bfloat16)

    def slab_grad(slab):
        flat = slab.reshape(-1, samples)
        product = lax.dot_general(flat, grad_pre_one, (((1,), (1,)), ((), ())), preferred_element_type=jnp.float32)
        return (product / samples).astype(jnp.bfloat16).reshape(dense_one.shape[1:])
    grad_dense_one = lax.map(slab_grad, pooled)
    grad_features = jnp.dot(weights_flat, grad_pre_one, preferred_element_type=jnp.float32).astype(jnp.bfloat16)
    grad_blocks = split_samples(grad_features.reshape(pooled.shape), block_count, block_size)

    def backward_block(pair):
        padded, grad_pooled = pair
        conv_out = conv_forward(padded, conv_kernel)
        grad_out = (spread(grad_pooled.astype(jnp.float32)) / 8.0 * leaky_derivative(conv_out)).astype(jnp.bfloat16)
        grad_padded = jnp.pad(grad_out, rim)
        grad_input = conv_back_input(grad_padded, conv_kernel).astype(jnp.bfloat16)
        return (grad_input, conv_back_kernel(padded, grad_out))
    grad_inputs, grad_kernels = lax.map(backward_block, (blocks, grad_blocks))
    grad_conv = lax.optimization_barrier(jnp.sum(grad_kernels, axis=0)) / samples
    grad_volume = join_samples(grad_inputs)
    return (prediction, grad_dense_one, grad_conv, grad_volume)
```

```python
import jax
import jax.numpy as jnp
from jax import lax
from jax.sharding import PartitionSpec as P

loss_scale = 1024.0
leak_slope = 0.3


def with_halo(array, sides, width):
    for axis, dim in sides:
        size, length = (lax.axis_size(axis), array.shape[dim])
        up = [(i, (i + 1) % size) for i in range(size - 1)]
        down = [(j, i) for i, j in up]
        last = lax.slice_in_dim(array, length - width, length, axis=dim)
        initial = lax.slice_in_dim(array, 0, width, axis=dim)
        before = lax.ppermute(last, axis, up)
        after = lax.ppermute(initial, axis, down)
        array = jnp.concatenate([before, array, after], axis=dim)
    return array


def from_behind(block, axis, distance):
    devices = range(lax.axis_size(axis))
    route = [(i - distance, i) for i in devices if i - distance in devices]
    return lax.ppermute(block, axis, route)


def shortened(array):
    return jax.tree.map(lambda a: a.astype(jnp.bfloat16) if a.dtype == jnp.float32 else a, array)


def smooth_leaky(values):
    return leak_slope * values + (1.0 - leak_slope) * jax.nn.softplus(values)


def leaky_derivative(values):
    return leak_slope + (1.0 - leak_slope) * jax.nn.sigmoid(values)


def conv_forward(padded, kernel):
    return lax.conv_general_dilated(
        padded,
        kernel,
        (1, 1, 1),
        "VALID",
        dimension_numbers=("DHWCN", "DHWIO", "DHWCN"),
        preferred_element_type=jnp.float32,
    )


def conv_back_input(padded_grad, kernel):
    flipped = kernel[::-1, ::-1, ::-1]
    return lax.conv_general_dilated(
        padded_grad,
        flipped,
        (1, 1, 1),
        "VALID",
        dimension_numbers=("DHWCN", "DHWOI", "DHWCN"),
        preferred_element_type=jnp.float32,
    )


def conv_back_kernel(padded, gradient):
    return lax.conv_general_dilated(
        padded,
        gradient,
        (1, 1, 1),
        "VALID",
        dimension_numbers=("DHWNC", "DHWOI", "DHWNC"),
        preferred_element_type=jnp.float32,
    )


def pooling(values):
    extent_x, extent_y, extent_z, channels, samples = values.shape
    return values.reshape(
        extent_x // 2, 2, extent_y // 2, 2, extent_z // 2, 2, channels, samples
    ).mean(axis=(1, 3, 5))


def spread(values):
    extent_x, extent_y, extent_z, channels, samples = values.shape
    widened = jnp.broadcast_to(
        values[:, None, :, None, :, None],
        (extent_x, 2, extent_y, 2, extent_z, 2, channels, samples),
    )
    return widened.reshape(2 * extent_x, 2 * extent_y, 2 * extent_z, channels, samples)


def fold_faces(inner, from_below, from_above, axis_dim):
    length = inner.shape[axis_dim]
    first = lax.slice_in_dim(inner, 0, 1, axis=axis_dim) + from_below
    middle = lax.slice_in_dim(inner, 1, length - 1, axis=axis_dim)
    last = lax.slice_in_dim(inner, length - 1, length, axis=axis_dim) + from_above
    return jnp.concatenate([first, middle, last], axis=axis_dim)


def body(volume, conv_kernel, dense_one, dense_two, dense_three, targets):
    padded = with_halo(volume, (("gx", 0), ("gy", 1), ("gz", 2)), 1)
    conv_out = conv_forward(padded, conv_kernel)
    pooled = pooling(smooth_leaky(conv_out)).astype(jnp.bfloat16)
    half_x, half_y, half_z, channels, samples = pooled.shape
    groups_y = lax.axis_size("gy")
    groups_z = lax.axis_size("gz")
    per_group = channels // (groups_y * groups_z)
    arrived = lax.all_to_all(pooled[None], ("gy", "gz"), split_axis=4, concat_axis=0, tiled=True)
    arrived = arrived.reshape(groups_y, groups_z, half_x, half_y, half_z, per_group, samples)
    weights_local = dense_one.reshape(
        half_x, groups_y, half_y, groups_z, half_z, per_group, dense_one.shape[4]
    )
    partial_one = jnp.einsum(
        "uvxyzcb,xuyvzch->bh", arrived, weights_local, preferred_element_type=jnp.float32
    )
    everyone = ("gx", "gy", "gz")
    devices = lax.axis_size(everyone)
    rows = partial_one.shape[1] // 128
    shares = partial_one.astype(jnp.bfloat16).reshape(devices, rows, 128)
    gathered = lax.all_to_all(shares, everyone, split_axis=0, concat_axis=0, tiled=True)
    pre_one = gathered.astype(jnp.float32).sum(axis=0).reshape(1, rows * 128)
    mine = lax.axis_index(everyone)
    target = lax.dynamic_slice_in_dim(targets, mine, 1, axis=1).T
    hidden_one = smooth_leaky(pre_one)
    pre_two = jnp.dot(hidden_one, dense_two, precision=lax.Precision.HIGHEST)
    hidden_two = smooth_leaky(pre_two)
    own_prediction = jnp.dot(hidden_two, dense_three, precision=lax.Precision.HIGHEST)
    error_grad = loss_scale * (own_prediction - target)
    grad_pre_two = jnp.dot(
        error_grad, dense_three.T, precision=lax.Precision.HIGHEST
    ) * leaky_derivative(pre_two)
    own_grad = (
        jnp.dot(grad_pre_two, dense_two.T, precision=lax.Precision.HIGHEST)
        * leaky_derivative(pre_one)
    ).astype(jnp.bfloat16)
    copies = jnp.broadcast_to(own_grad.reshape(1, rows, 128), (devices, rows, 128))
    grad_pre_one = lax.all_to_all(copies, everyone, split_axis=0, concat_axis=0, tiled=True)
    grad_pre_one = grad_pre_one.reshape(samples, rows * 128)
    grad_local = jnp.einsum(
        "uvxyzcb,bh->xuyvzch", arrived, grad_pre_one, preferred_element_type=jnp.float32
    )
    grad_dense_one = (grad_local / samples).astype(jnp.bfloat16).reshape(dense_one.shape)
    grad_arrived = jnp.einsum(
        "xuyvzch,bh->uvxyzcb", weights_local, grad_pre_one, preferred_element_type=jnp.float32
    ).astype(jnp.bfloat16)
    outgoing = grad_arrived.reshape(groups_y * groups_z, half_x, half_y, half_z, per_group, samples)
    returned = lax.all_to_all(outgoing, ("gy", "gz"), split_axis=0, concat_axis=4, tiled=True)
    grad_pooled = returned.reshape(half_x, half_y, half_z, channels, samples)
    grad_out = (spread(grad_pooled.astype(jnp.float32)) / 8.0 * leaky_derivative(conv_out)).astype(
        jnp.bfloat16
    )
    widened = jnp.pad(grad_out, ((2, 2), (2, 2), (2, 2), (0, 0), (0, 0)))
    whole = conv_back_input(widened, conv_kernel)
    below_x = from_behind(whole[-1:].astype(jnp.bfloat16), "gx", 1).astype(jnp.float32)
    above_x = from_behind(whole[:1].astype(jnp.bfloat16), "gx", -1).astype(jnp.float32)
    folded = fold_faces(whole[1:-1], below_x, above_x, 0)
    below_y = from_behind(shortened(folded[:, -1:]), "gy", 1)
    above_y = from_behind(shortened(folded[:, :1]), "gy", -1)
    folded = fold_faces(folded[:, 1:-1], below_y, above_y, 1)
    below_z = from_behind(shortened(folded[:, :, -1:]), "gz", 1)
    above_z = from_behind(shortened(folded[:, :, :1]), "gz", -1)
    folded = fold_faces(folded[:, :, 1:-1], below_z, above_z, 2)
    grad_volume = folded.astype(jnp.bfloat16)
    kernel_local = conv_back_kernel(padded, grad_out)
    share = kernel_local.size // devices
    pieces = jnp.pad(kernel_local.reshape(devices, share), ((0, 0), (0, 512 - share)))
    pieces = lax.all_to_all(
        pieces.reshape(devices, 4, 128), everyone, split_axis=0, concat_axis=0, tiled=True
    )
    own_piece = (pieces.sum(axis=0) / samples).reshape(512)
    own_piece = jnp.concatenate(
        [own_piece[:share], own_prediction.reshape(-1), jnp.zeros((508 - share,), jnp.float32)]
    )
    results = jnp.broadcast_to(own_piece.reshape(1, 4, 128), (devices, 4, 128))
    results = lax.all_to_all(results, everyone, split_axis=0, concat_axis=0, tiled=True)
    results = results.reshape(devices, 512)
    grad_conv = results[:, :share].reshape(conv_kernel.shape)
    prediction = results[:, share : share + 4].T
    return (prediction, grad_dense_one, grad_conv, grad_volume)


def solution(mesh):
    return jax.shard_map(
        body,
        mesh=mesh,
        in_specs=(
            P("gx", "gy", "gz", None, None),
            P(),
            P("gx", None, None, ("gy", "gz"), None),
            P(),
            P(),
            P(),
        ),
        out_specs=(
            P(),
            P("gx", None, None, ("gy", "gz"), None),
            P(),
            P("gx", "gy", "gz", None, None),
        ),
        check_vma=False,
    )
```

```python
import jax
import jax.numpy as jnp
from jax import lax
from jax.experimental import pallas as pl
from jax.experimental.pallas import tpu as pltpu
from jax.sharding import PartitionSpec as P

loss_scale = 1024.0
leak_slope = 0.3
everyone = ("gx", "gy", "gz")
bf16 = jnp.bfloat16
f32 = jnp.float32


def in_hbm(array):
    return pltpu.with_memory_space_constraint(array, pltpu.HBM)


def neighbours(axis):
    size = lax.axis_size(axis)
    up = [(i, i + 1) for i in range(size - 1)]
    return up, [(j, i) for i, j in up]


def both_ways(toward_up, toward_down, axis):
    up, down = neighbours(axis)
    return lax.ppermute(toward_up, axis, up), lax.ppermute(toward_down, axis, down)


def smooth_leaky(values):
    return leak_slope * values + (1.0 - leak_slope) * jax.nn.softplus(values)


def leaky_derivative(values):
    return leak_slope + (1.0 - leak_slope) * jax.nn.sigmoid(values)


def banded_kernel(kernel, cells):
    taps_x, taps_y, _, c_in, c_out = kernel.shape
    bands = [
        jnp.pad(kernel, ((0, 0), (0, 0), (z, cells - 1 - z), (0, 0), (0, 0)))
        for z in range(cells)
    ]
    whole = jnp.stack(bands)
    return jnp.transpose(whole, (3, 4, 1, 2, 0, 5)).reshape(
        (cells + 2) * c_in, taps_x * taps_y * cells * c_out
    )


def forward_call(core, x_lo, x_hi, y_lo, y_hi, z_lo, z_hi, twice):
    nx, ny, width, lanes = core.shape
    edge = z_lo.shape[2]
    depth = width + 2 * edge
    half = twice.shape[1] // 2
    rows = 4 * half
    tap = 3 * edge

    def build(twice, matrix):
        for pair in range(2):
            for start in range(0, 9, 2):
                count = min(2, 9 - start)
                side = lax.broadcasted_iota(jnp.int32, (tap, 2 * half), 1) < half
                blocks = []
                for k in range(start, start + count):
                    block = twice[k * tap : (k + 1) * tap, :]
                    blocks.append(jnp.where(side, block, jnp.zeros_like(block)))
                    blocks.append(jnp.where(side, jnp.zeros_like(block), block))
                stacked = jnp.concatenate(blocks, axis=0)
                size = count * depth
                here = lax.broadcasted_iota(jnp.int32, (size, size), 0)
                from_row = lax.broadcasted_iota(jnp.int32, (size, size), 1)
                which = from_row // tap
                moved = (
                    (which // 2) * depth + (2 * pair + which % 2) * edge + from_row - which * tap
                )
                place = jnp.where(here == moved, 1.0, 0.0).astype(bf16)
                matrix[
                    pair * 2 * half : (pair + 1) * 2 * half,
                    start * depth : (start + count) * depth,
                ] = lax.dot_general(
                    stacked, place, (((0,), (1,)), ((), ())), preferred_element_type=f32
                ).astype(bf16)

    def body(
        core, x_lo, x_hi, y_lo, y_hi, z_lo, z_hi, twice, kept, conv_out, pooled, padded, matrix, sem
    ):
        step = pl.program_id(0)

        @pl.when(step == 0)
        def _():
            middle = pl.ds(edge, width)
            padded[1 : nx + 1, 1 : ny + 1, middle, :] = core[...]
            padded[0, 1 : ny + 1, middle, :] = x_lo[...]
            padded[nx + 1, 1 : ny + 1, middle, :] = x_hi[...]
            padded[:, 0, middle, :] = y_lo[...]
            padded[:, ny + 1, middle, :] = y_hi[...]
            padded[:, :, 0:edge, :] = z_lo[...]
            padded[:, :, edge + width : depth, :] = z_hi[...]
            pltpu.make_async_copy(padded, kept, sem).start()
            build(twice, matrix)

        weights = matrix[...]
        for pair in range(ny // 2):
            y = 2 * pair
            total = None
            for inner in range(2):
                x = 2 * step + inner
                patch = jnp.concatenate(
                    [
                        jnp.concatenate(
                            [padded[x + dx, y + dy], padded[x + dx, y + dy + 1]], axis=1
                        )
                        for dx in range(3)
                        for dy in range(3)
                    ],
                    axis=0,
                )
                values = jnp.dot(weights, patch, preferred_element_type=f32)
                conv_out[inner, y] = values[:, :lanes].astype(bf16)
                conv_out[inner, y + 1] = values[:, lanes:].astype(bf16)
                soft = jnp.maximum(values, 0.0) + jnp.log(1.0 + jnp.exp(-jnp.abs(values)))
                acted = leak_slope * values + (1.0 - leak_slope) * soft
                across = acted[:, :lanes] + acted[:, lanes:]
                total = across if total is None else total + across
            total = total * 0.125
            pooled[0, pair, 0] = (total[:half] + total[half : 2 * half]).astype(bf16)
            pooled[0, pair, 1] = (total[2 * half : 3 * half] + total[3 * half :]).astype(bf16)

        @pl.when(step == nx // 2 - 1)
        def _():
            pltpu.make_async_copy(padded, kept, sem).wait()

    def whole(array):
        return pl.BlockSpec(array.shape, lambda i: (0,) * array.ndim)

    operands = (in_hbm(core), x_lo, x_hi, y_lo, y_hi, z_lo, z_hi, twice)
    padded_shape = (nx + 2, ny + 2, depth, lanes)
    return pl.pallas_call(
        body,
        grid=(nx // 2,),
        in_specs=[whole(a) for a in operands],
        out_specs=[
            pl.BlockSpec(memory_space=pltpu.HBM),
            pl.BlockSpec((2, ny, rows, lanes), lambda i: (i, 0, 0, 0)),
            pl.BlockSpec((1, ny // 2, 2, half, lanes), lambda i: (i, 0, 0, 0, 0)),
        ],
        out_shape=[
            pltpu.HBM(padded_shape, bf16),
            pltpu.HBM((nx, ny, rows, lanes), bf16),
            jax.ShapeDtypeStruct((nx // 2, ny // 2, 2, half, lanes), bf16),
        ],
        scratch_shapes=[
            pltpu.VMEM(padded_shape, bf16),
            pltpu.VMEM((rows, 9 * depth), bf16),
            pltpu.SemaphoreType.DMA,
        ],
        compiler_params=pltpu.CompilerParams(vmem_limit_bytes=40 * 2**20),
        cost_estimate=pl.CostEstimate(flops=7 * 10**9, bytes_accessed=16 * 2**20, transcendentals=0),
        name="conv_forward",
    )(*operands)


def kernel_grad_call(padded, conv_out, grad_pooled, c_in):
    nx, ny, rows, lanes = conv_out.shape
    depth = padded.shape[2]
    c_out = rows // 4

    def body(rows_0, rows_1, conv_out, grad_pooled, grad_out, result, sums):
        step = pl.program_id(0)

        @pl.when(step == 0)
        def _():
            sums[...] = jnp.zeros(sums.shape, f32)

        for x in range(2):
            for y in range(ny):
                values = conv_out[x, y].astype(f32)
                rise = (1.0 - leak_slope) / 16.0
                slope = (leak_slope / 8.0 + rise) + rise * jnp.tanh(0.5 * values)
                pieces = [grad_pooled[0, y // 2, z // 2].astype(f32) for z in range(4)]
                grad_out[x, y] = (jnp.concatenate(pieces, axis=0) * slope).astype(bf16)
        layers = [rows_0.at[0], rows_0.at[1], rows_1.at[0], rows_1.at[1]]
        right = jnp.concatenate(
            [grad_out[x, y] for x in range(2) for y in range(ny)], axis=1
        )
        for dx in range(3):
            left = jnp.concatenate(
                [
                    jnp.concatenate(
                        [layers[x + dx][y + dy] for x in range(2) for y in range(ny)], axis=1
                    )
                    for dy in range(3)
                ],
                axis=0,
            )
            sums[dx] += lax.dot_general(
                left, right, (((1,), (1,)), ((), ())), preferred_element_type=f32
            )

        @pl.when(step == nx // 2 - 1)
        def _():
            for dx in range(3):
                for dy in range(3):
                    for dz in range(3):
                        total = None
                        for z in range(4):
                            start = dy * depth + (z + dz) * c_in
                            piece = sums[dx, start : start + c_in, z * c_out : (z + 1) * c_out]
                            total = piece if total is None else total + piece
                        result[9 * dx + 3 * dy + dz] = total

    return pl.pallas_call(
        body,
        grid=(nx // 2,),
        in_specs=[
            pl.BlockSpec((2,) + padded.shape[1:], lambda i: (i, 0, 0, 0)),
            pl.BlockSpec((2,) + padded.shape[1:], lambda i: (i + 1, 0, 0, 0)),
            pl.BlockSpec((2, ny, rows, lanes), lambda i: (i, 0, 0, 0)),
            pl.BlockSpec((1,) + grad_pooled.shape[1:], lambda i: (i, 0, 0, 0, 0)),
        ],
        out_specs=[
            pl.BlockSpec((2, ny, rows, lanes), lambda i: (i, 0, 0, 0)),
            pl.BlockSpec((27, c_in, c_out), lambda i: (0, 0, 0)),
        ],
        out_shape=[
            pltpu.HBM((nx, ny, rows, lanes), bf16),
            jax.ShapeDtypeStruct((27, c_in, c_out), f32),
        ],
        scratch_shapes=[pltpu.VMEM((3, 3 * depth, rows), f32)],
        compiler_params=pltpu.CompilerParams(vmem_limit_bytes=32 * 2**20),
        cost_estimate=pl.CostEstimate(flops=8 * 10**9, bytes_accessed=14 * 2**20, transcendentals=0),
        name="conv_kernel_grad",
    )(in_hbm(padded), in_hbm(padded), in_hbm(conv_out), grad_pooled)


def input_grad_call(grad_out, matrix):
    nx, ny, rows, lanes = grad_out.shape
    depth = matrix.shape[0]

    def body(grad_out, matrix, spread, held):
        step = pl.program_id(0)

        @pl.when(step == 0)
        def _():
            for edge in (0, nx + 2):
                held[edge : edge + 2] = jnp.zeros((2,) + held.shape[1:], bf16)
            for edge in (0, ny + 2):
                held[2 : nx + 2, edge : edge + 2] = jnp.zeros((nx, 2, rows, lanes), bf16)

        @pl.when(step < nx // 2)
        def _():
            held[pl.ds(2 * step + 2, 2), 2 : ny + 2] = grad_out[...]

        for x in range(2):
            at = 2 * step + 2 + x
            for pair in range((ny + 2) // 2):
                y = 2 * pair
                taps = [dy for dy in range(3) if y + 1 - dy >= 0 and y - dy < ny]
                values = None
                for dx in range(3):
                    patch = jnp.concatenate(
                        [
                            jnp.concatenate(
                                [held[at - dx, y + 2 - dy], held[at - dx, y + 3 - dy]], axis=1
                            )
                            for dy in taps
                        ],
                        axis=0,
                    )
                    start = (3 * dx + taps[0]) * rows
                    term = jnp.dot(
                        matrix[:, start : start + len(taps) * rows],
                        patch,
                        preferred_element_type=f32,
                    )
                    values = term if values is None else values + term
                values = values.astype(bf16)
                spread[x, y] = values[:, :lanes]
                spread[x, y + 1] = values[:, lanes:]

    return pl.pallas_call(
        body,
        grid=(nx // 2 + 1,),
        in_specs=[
            pl.BlockSpec((2, ny, rows, lanes), lambda i: (jnp.minimum(i, nx // 2 - 1), 0, 0, 0)),
            pl.BlockSpec(matrix.shape, lambda i: (0, 0)),
        ],
        out_specs=pl.BlockSpec((2, ny + 2, depth, lanes), lambda i: (i, 0, 0, 0)),
        out_shape=pltpu.HBM((nx + 2, ny + 2, depth, lanes), bf16),
        scratch_shapes=[pltpu.VMEM((nx + 4, ny + 4, rows, lanes), bf16)],
        compiler_params=pltpu.CompilerParams(vmem_limit_bytes=40 * 2**20),
        cost_estimate=pl.CostEstimate(flops=9 * 10**9, bytes_accessed=12 * 2**20, transcendentals=0),
        name="conv_input_grad",
    )(in_hbm(grad_out), matrix)


def finish_call(spread, x_lo, x_hi, y_lo, y_hi, z_lo, z_hi):
    nx, ny, edge, lanes = z_lo.shape
    depth = spread.shape[2]
    width = depth - 2 * edge

    def body(spread_0, spread_1, x_lo, x_hi, y_lo, y_hi, z_lo, z_hi, result):
        step = pl.program_id(0)
        middle = slice(edge, edge + width)

        def base(x, y):
            value = (spread_0, spread_1)[x][0, y + 1, middle].astype(f32)
            if y == 0:
                value = value + y_lo[x, middle].astype(f32)
            if y == ny - 1:
                value = value + y_hi[x, middle].astype(f32)
            low = value[:edge] + z_lo[x, y].astype(f32)
            high = value[width - edge :] + z_hi[x, y].astype(f32)
            return jnp.concatenate([low, value[edge : width - edge], high], axis=0)

        def write(x, term):
            for y in range(ny):
                value = base(x, y)
                if term is not None:
                    value = value + term[y + 1, middle].astype(f32)
                result[x, y] = value.astype(bf16)

        @pl.when(step == 0)
        def _():
            write(0, x_lo)

        @pl.when(step > 0)
        def _():
            write(0, None)

        @pl.when(step == nx // 2 - 1)
        def _():
            write(1, x_hi)

        @pl.when(step < nx // 2 - 1)
        def _():
            write(1, None)

    def whole(array):
        return pl.BlockSpec(array.shape, lambda i: (0,) * array.ndim)

    def sliced(array):
        return pl.BlockSpec((2,) + array.shape[1:], lambda i: (i,) + (0,) * (array.ndim - 1))

    return pl.pallas_call(
        body,
        grid=(nx // 2,),
        in_specs=[
            pl.BlockSpec((1,) + spread.shape[1:], lambda i: (2 * i + 1, 0, 0, 0)),
            pl.BlockSpec((1,) + spread.shape[1:], lambda i: (2 * i + 2, 0, 0, 0)),
            whole(x_lo),
            whole(x_hi),
            sliced(y_lo),
            sliced(y_hi),
            sliced(z_lo),
            sliced(z_hi),
        ],
        out_specs=pl.BlockSpec((2, ny, width, lanes), lambda i: (i, 0, 0, 0)),
        out_shape=jax.ShapeDtypeStruct((nx, ny, width, lanes), bf16),
        compiler_params=pltpu.CompilerParams(vmem_limit_bytes=24 * 2**20),
        cost_estimate=pl.CostEstimate(flops=10**8, bytes_accessed=10 * 2**20, transcendentals=0),
        name="fold_faces",
    )(
        in_hbm(spread),
        in_hbm(spread),
        x_lo,
        x_hi,
        in_hbm(y_lo),
        in_hbm(y_hi),
        in_hbm(z_lo),
        in_hbm(z_hi),
    )


def exchange(array, axes):
    return lax.all_to_all(array, axes, split_axis=0, concat_axis=0, tiled=True)


def body(volume, conv_kernel, dense_one, dense_two, dense_three, targets):
    nx, ny, nz, c_in, samples = volume.shape
    c_out = conv_kernel.shape[4]
    groups_y = lax.axis_size("gy")
    groups_z = lax.axis_size("gz")
    groups = groups_y * groups_z
    devices = lax.axis_size(everyone)
    per_group = c_out // groups

    core = volume.reshape(nx, ny, nz * c_in, samples)
    x_lo, x_hi = both_ways(core[-1:], core[:1], "gx")
    first = jnp.concatenate([x_lo[:, :1], core[:, :1], x_hi[:, :1]], axis=0)
    last = jnp.concatenate([x_lo[:, -1:], core[:, -1:], x_hi[:, -1:]], axis=0)
    y_lo, y_hi = both_ways(last, first, "gy")

    def z_layer(rows):
        sides = [a[:, :, rows] for a in (y_lo, x_lo, core, x_hi, y_hi)]
        middle = jnp.concatenate(sides[1:4], axis=0)
        return jnp.concatenate([sides[0], middle, sides[4]], axis=1)

    z_lo, z_hi = both_ways(z_layer(slice(-c_in, None)), z_layer(slice(0, c_in)), "gz")
    backward_matrix = banded_kernel(conv_kernel, nz)
    twice = conv_kernel.reshape(-1, c_out)
    twice = jnp.concatenate([twice, twice], axis=1)
    padded, conv_out, pooled = forward_call(
        core, x_lo[0], x_hi[0], y_lo[:, 0], y_hi[:, 0], z_lo, z_hi, twice
    )

    half_x, half_y, half_z = nx // 2, ny // 2, nz // 2
    cells = half_x * half_y * half_z
    outgoing = pooled.reshape(cells, groups, per_group, samples).transpose(1, 0, 2, 3)
    arrived = exchange(outgoing.reshape(groups, cells * per_group, samples), ("gy", "gz"))
    arrived = arrived.reshape(groups_y, groups_z, half_x, half_y, half_z, per_group, samples)
    features = arrived.transpose(2, 0, 3, 1, 4, 5, 6).reshape(-1, samples)
    weights = lax.optimization_barrier(dense_one.reshape(-1, dense_one.shape[4]))
    partial_one = lax.dot_general(
        features, weights, (((0,), (0,)), ((), ())), preferred_element_type=f32
    )
    rows = partial_one.shape[1] // 128
    gathered = exchange(partial_one.astype(bf16).reshape(devices, rows, 128), everyone)
    pre_one = gathered.astype(f32).sum(axis=0).reshape(1, rows * 128)
    mine = lax.axis_index(everyone)
    target = lax.dynamic_slice_in_dim(targets, mine, 1, axis=1).T
    hidden_one = smooth_leaky(pre_one)
    pre_two = jnp.dot(hidden_one, dense_two, precision=lax.Precision.HIGHEST)
    hidden_two = smooth_leaky(pre_two)
    own_prediction = jnp.dot(hidden_two, dense_three, precision=lax.Precision.HIGHEST)
    error_grad = loss_scale * (own_prediction - target)
    grad_pre_two = jnp.dot(
        error_grad, dense_three.T, precision=lax.Precision.HIGHEST
    ) * leaky_derivative(pre_two)
    own_grad = (
        jnp.dot(grad_pre_two, dense_two.T, precision=lax.Precision.HIGHEST)
        * leaky_derivative(pre_one)
    ).astype(bf16)
    copies = jnp.broadcast_to(own_grad.reshape(1, rows, 128), (devices, rows, 128))
    grad_pre_one = exchange(copies, everyone).reshape(samples, rows * 128)

    grad_features = lax.dot_general(
        weights, grad_pre_one, (((1,), (1,)), ((), ())), preferred_element_type=f32
    ).astype(bf16)
    grad_features = grad_features.reshape(
        half_x, groups_y, half_y, groups_z, half_z, per_group, samples
    ).transpose(1, 3, 0, 2, 4, 5, 6)
    returned = exchange(grad_features.reshape(groups, cells * per_group, samples), ("gy", "gz"))
    grad_dense_one = (
        jnp.einsum("uvxyzcb,bh->xuyvzch", arrived, grad_pre_one, preferred_element_type=f32)
        / samples
    ).astype(bf16).reshape(dense_one.shape)
    grad_pooled = (
        returned.reshape(groups, cells, per_group, samples).transpose(1, 0, 2, 3)
    ).reshape(pooled.shape)

    grad_out, kernel_local = kernel_grad_call(padded, conv_out, grad_pooled, c_in)
    spread = input_grad_call(grad_out, backward_matrix)
    from_lo, from_hi = both_ways(spread[-1], spread[0], "gx")

    def added(array, first_term, last_term):
        head = (array[:1].astype(f32) + first_term.astype(f32)).astype(bf16)
        tail = (array[-1:].astype(f32) + last_term.astype(f32)).astype(bf16)
        return jnp.concatenate([head, array[1:-1], tail], axis=0)

    y_down = added(spread[1:-1, 0], from_lo[None, 0], from_hi[None, 0])
    y_up = added(spread[1:-1, -1], from_lo[None, -1], from_hi[None, -1])
    y_lo_terms, y_hi_terms = both_ways(y_up, y_down, "gy")

    def with_edges(part):
        face = spread[1:-1, 1:-1, part]
        face = added(face, from_lo[None, 1:-1, part], from_hi[None, 1:-1, part])
        head = (face[:, :1].astype(f32) + y_lo_terms[:, None, part].astype(f32)).astype(bf16)
        tail = (face[:, -1:].astype(f32) + y_hi_terms[:, None, part].astype(f32)).astype(bf16)
        return jnp.concatenate([head, face[:, 1:-1], tail], axis=1)

    z_down = with_edges(slice(0, c_in))
    z_up = with_edges(slice(-c_in, None))
    z_lo_terms, z_hi_terms = both_ways(z_up, z_down, "gz")
    grad_volume = finish_call(
        spread, from_lo, from_hi, y_lo_terms, y_hi_terms, z_lo_terms, z_hi_terms
    ).reshape(volume.shape)

    share = kernel_local.size // devices
    pieces = jnp.pad(kernel_local.reshape(devices, share), ((0, 0), (0, 512 - share)))
    pieces = exchange(pieces.reshape(devices, 4, 128), everyone)
    own_piece = (pieces.sum(axis=0) / samples).reshape(512)
    own_piece = jnp.concatenate(
        [own_piece[:share], own_prediction.reshape(-1), jnp.zeros((508 - share,), f32)]
    )
    results = exchange(
        jnp.broadcast_to(own_piece.reshape(1, 4, 128), (devices, 4, 128)), everyone
    ).reshape(devices, 512)
    grad_conv = results[:, :share].reshape(conv_kernel.shape)
    prediction = results[:, share : share + 4].T
    return (prediction, grad_dense_one, grad_conv, grad_volume)


def solution(mesh):
    return jax.shard_map(
        body,
        mesh=mesh,
        in_specs=(
            P("gx", "gy", "gz", None, None),
            P(),
            P("gx", None, None, ("gy", "gz"), None),
            P(),
            P(),
            P(),
        ),
        out_specs=(
            P(),
            P("gx", None, None, ("gy", "gz"), None),
            P(),
            P("gx", "gy", "gz", None, None),
        ),
        check_vma=False,
    )
```

```python
import jax
import jax.numpy as jnp
from jax import lax
from jax.experimental import pallas as pl
from jax.experimental.pallas import tpu as pltpu
from jax.sharding import PartitionSpec as P

loss_scale = 1024.0
leak_slope = 0.3
everyone = ("gx", "gy", "gz")
bf16 = jnp.bfloat16
f32 = jnp.float32


def in_hbm(array):
    return pltpu.with_memory_space_constraint(array, pltpu.HBM)


def neighbours(axis):
    size = lax.axis_size(axis)
    up = [(i, i + 1) for i in range(size - 1)]
    return up, [(j, i) for i, j in up]


def both_ways(toward_up, toward_down, axis):
    up, down = neighbours(axis)
    return lax.ppermute(toward_up, axis, up), lax.ppermute(toward_down, axis, down)


def smooth_leaky(values):
    return leak_slope * values + (1.0 - leak_slope) * jax.nn.softplus(values)


def leaky_derivative(values):
    return leak_slope + (1.0 - leak_slope) * jax.nn.sigmoid(values)


def banded_matrices(twice, cells, c_in):
    lanes = twice.shape[1]
    half = lanes // 2
    tap = 3 * c_in
    depth = (cells + 2) * c_in
    rows = cells * half

    def body(twice, forward, backward):
        side = lax.broadcasted_iota(jnp.int32, (tap, lanes), 1) < half
        for pair in range(cells // 2):
            for start in range(0, 9, 2):
                count = min(2, 9 - start)
                blocks = []
                for k in range(start, start + count):
                    block = twice[k * tap : (k + 1) * tap, :]
                    blocks.append(jnp.where(side, block, jnp.zeros_like(block)))
                    blocks.append(jnp.where(side, jnp.zeros_like(block), block))
                stacked = jnp.concatenate(blocks, axis=0)
                size = count * depth
                here = lax.broadcasted_iota(jnp.int32, (size, size), 0)
                from_row = lax.broadcasted_iota(jnp.int32, (size, size), 1)
                which = from_row // tap
                moved = (
                    (which // 2) * depth + (2 * pair + which % 2) * c_in + from_row - which * tap
                )
                place = jnp.where(here == moved, 1.0, 0.0).astype(bf16)
                forward[
                    pair * lanes : (pair + 1) * lanes, start * depth : (start + count) * depth
                ] = lax.dot_general(
                    stacked, place, (((0,), (1,)), ((), ())), preferred_element_type=f32
                ).astype(bf16)
                both = jnp.dot(place, stacked, preferred_element_type=f32).astype(bf16)
                for k in range(count):
                    at = (start + k) * rows + pair * lanes
                    backward[:, at : at + lanes] = both[k * depth : (k + 1) * depth]

    return pl.pallas_call(
        body,
        out_shape=[
            jax.ShapeDtypeStruct((rows, 9 * depth), bf16),
            jax.ShapeDtypeStruct((depth, 9 * rows), bf16),
        ],
        compiler_params=pltpu.CompilerParams(vmem_limit_bytes=16 * 2**20),
        cost_estimate=pl.CostEstimate(flops=10**9, bytes_accessed=2**21, transcendentals=0),
        name="banded_matrices",
    )(twice)


def forward_call(core, x_lo, x_hi, y_lo, y_hi, z_lo, z_hi, matrix):
    nx, ny, width, lanes = core.shape
    edge = z_lo.shape[2]
    depth = width + 2 * edge
    rows = matrix.shape[0]
    half = rows // 4

    def body(
        core, x_lo, x_hi, y_lo, y_hi, z_lo, z_hi, matrix, kept, conv_out, pooled, padded, sem
    ):
        step = pl.program_id(0)

        @pl.when(step == 0)
        def _():
            middle = pl.ds(edge, width)
            padded[1 : nx + 1, 1 : ny + 1, middle, :] = core[...]
            padded[0, 1 : ny + 1, middle, :] = x_lo[...]
            padded[nx + 1, 1 : ny + 1, middle, :] = x_hi[...]
            padded[:, 0, middle, :] = y_lo[...]
            padded[:, ny + 1, middle, :] = y_hi[...]
            padded[:, :, 0:edge, :] = z_lo[...]
            padded[:, :, edge + width : depth, :] = z_hi[...]
            pltpu.make_async_copy(padded, kept, sem).start()

        weights = matrix[...]
        for pair in range(ny // 2):
            y = 2 * pair
            total, factor = 0.0, 1.0
            for inner in range(2):
                x = 2 * step + inner
                patch = jnp.concatenate(
                    [
                        jnp.concatenate(
                            [padded[x + dx, y + dy], padded[x + dx, y + dy + 1]], axis=1
                        )
                        for dx in range(3)
                        for dy in range(3)
                    ],
                    axis=0,
                )
                values = jnp.dot(weights, patch, preferred_element_type=f32)
                conv_out[inner, y] = values[:, :lanes].astype(bf16)
                conv_out[inner, y + 1] = values[:, lanes:].astype(bf16)
                straight = jnp.maximum(leak_slope * values, values)
                grown = 1.0 + jnp.exp(-jnp.abs(values))
                total = total + (straight[:, :lanes] + straight[:, lanes:])
                factor = factor * (grown[:, :lanes] * grown[:, lanes:])
            for z in range(2):
                low, high = 2 * z * half, (2 * z + 1) * half
                bent = jnp.log(factor[low : low + half] * factor[high : high + half])
                mean = 0.125 * (total[low : low + half] + total[high : high + half])
                pooled[0, pair, z] = (mean + (0.125 * (1.0 - leak_slope)) * bent).astype(bf16)

        @pl.when(step == nx // 2 - 1)
        def _():
            pltpu.make_async_copy(padded, kept, sem).wait()

    def whole(array):
        return pl.BlockSpec(array.shape, lambda i: (0,) * array.ndim)

    operands = (in_hbm(core), x_lo, x_hi, y_lo, y_hi, z_lo, z_hi, matrix)
    padded_shape = (nx + 2, ny + 2, depth, lanes)
    return pl.pallas_call(
        body,
        grid=(nx // 2,),
        in_specs=[whole(a) for a in operands],
        out_specs=[
            pl.BlockSpec(memory_space=pltpu.HBM),
            pl.BlockSpec((2, ny, rows, lanes), lambda i: (i, 0, 0, 0)),
            pl.BlockSpec((1, ny // 2, 2, half, lanes), lambda i: (i, 0, 0, 0, 0)),
        ],
        out_shape=[
            pltpu.HBM(padded_shape, bf16),
            pltpu.HBM((nx, ny, rows, lanes), bf16),
            jax.ShapeDtypeStruct((nx // 2, ny // 2, 2, half, lanes), bf16),
        ],
        scratch_shapes=[
            pltpu.VMEM(padded_shape, bf16),
            pltpu.SemaphoreType.DMA,
        ],
        compiler_params=pltpu.CompilerParams(vmem_limit_bytes=40 * 2**20),
        cost_estimate=pl.CostEstimate(flops=7 * 10**9, bytes_accessed=16 * 2**20, transcendentals=0),
        name="conv_forward",
    )(*operands)


def kernel_grad_call(padded, conv_out, grad_pooled, c_in):
    nx, ny, rows, lanes = conv_out.shape
    depth = padded.shape[2]
    c_out = rows // 4

    def body(rows_0, rows_1, conv_out, grad_pooled, grad_out, result, sums):
        step = pl.program_id(0)

        @pl.when(step == 0)
        def _():
            sums[...] = jnp.zeros(sums.shape, f32)

        for x in range(2):
            for y in range(ny):
                values = conv_out[x, y].astype(f32)
                rise = (1.0 - leak_slope) / 16.0
                slope = (leak_slope / 8.0 + rise) + rise * jnp.tanh(0.5 * values)
                pieces = [grad_pooled[0, y // 2, z // 2].astype(f32) for z in range(4)]
                grad_out[x, y] = (jnp.concatenate(pieces, axis=0) * slope).astype(bf16)
        layers = [rows_0.at[0], rows_0.at[1], rows_1.at[0], rows_1.at[1]]
        right = jnp.concatenate(
            [grad_out[x, y] for x in range(2) for y in range(ny)], axis=1
        )
        for dx in range(3):
            left = jnp.concatenate(
                [
                    jnp.concatenate(
                        [layers[x + dx][y + dy] for x in range(2) for y in range(ny)], axis=1
                    )
                    for dy in range(3)
                ],
                axis=0,
            )
            sums[dx] += lax.dot_general(
                left, right, (((1,), (1,)), ((), ())), preferred_element_type=f32
            )

        @pl.when(step == nx // 2 - 1)
        def _():
            for dx in range(3):
                for dy in range(3):
                    for dz in range(3):
                        total = None
                        for z in range(4):
                            start = dy * depth + (z + dz) * c_in
                            piece = sums[dx, start : start + c_in, z * c_out : (z + 1) * c_out]
                            total = piece if total is None else total + piece
                        result[9 * dx + 3 * dy + dz] = total

    return pl.pallas_call(
        body,
        grid=(nx // 2,),
        in_specs=[
            pl.BlockSpec((2,) + padded.shape[1:], lambda i: (i, 0, 0, 0)),
            pl.BlockSpec((2,) + padded.shape[1:], lambda i: (i + 1, 0, 0, 0)),
            pl.BlockSpec((2, ny, rows, lanes), lambda i: (i, 0, 0, 0)),
            pl.BlockSpec((1,) + grad_pooled.shape[1:], lambda i: (i, 0, 0, 0, 0)),
        ],
        out_specs=[
            pl.BlockSpec((2, ny, rows, lanes), lambda i: (i, 0, 0, 0)),
            pl.BlockSpec((27, c_in, c_out), lambda i: (0, 0, 0)),
        ],
        out_shape=[
            pltpu.HBM((nx, ny, rows, lanes), bf16),
            jax.ShapeDtypeStruct((27, c_in, c_out), f32),
        ],
        scratch_shapes=[pltpu.VMEM((3, 3 * depth, rows), f32)],
        compiler_params=pltpu.CompilerParams(vmem_limit_bytes=32 * 2**20),
        cost_estimate=pl.CostEstimate(flops=8 * 10**9, bytes_accessed=14 * 2**20, transcendentals=0),
        name="conv_kernel_grad",
    )(in_hbm(padded), in_hbm(padded), in_hbm(conv_out), grad_pooled)


def input_grad_call(grad_out, matrix):
    nx, ny, rows, lanes = grad_out.shape
    depth = matrix.shape[0]

    def body(grad_out, matrix, spread, faces, held):
        step = pl.program_id(0)

        @pl.when(step == 0)
        def _():
            for edge in (0, nx + 2):
                held[edge : edge + 2] = jnp.zeros((2,) + held.shape[1:], bf16)
            for edge in (0, ny + 2):
                held[2 : nx + 2, edge : edge + 2] = jnp.zeros((nx, 2, rows, lanes), bf16)

        @pl.when(step < nx // 2)
        def _():
            held[pl.ds(2 * step + 2, 2), 2 : ny + 2] = grad_out[...]

        for x in range(2):
            at = 2 * step + 2 + x
            for pair in range((ny + 2) // 2):
                y = 2 * pair
                taps = [dy for dy in range(3) if y + 1 - dy >= 0 and y - dy < ny]
                values = None
                for dx in range(3):
                    patch = jnp.concatenate(
                        [
                            jnp.concatenate(
                                [held[at - dx, y + 2 - dy], held[at - dx, y + 3 - dy]], axis=1
                            )
                            for dy in taps
                        ],
                        axis=0,
                    )
                    start = (3 * dx + taps[0]) * rows
                    term = jnp.dot(
                        matrix[:, start : start + len(taps) * rows],
                        patch,
                        preferred_element_type=f32,
                    )
                    values = term if values is None else values + term
                values = values.astype(bf16)
                spread[x, y] = values[:, :lanes]
                spread[x, y + 1] = values[:, lanes:]
        faces[0] = jnp.where(step == 0, spread[0], spread[1])

    return pl.pallas_call(
        body,
        grid=(nx // 2 + 1,),
        in_specs=[
            pl.BlockSpec((2, ny, rows, lanes), lambda i: (jnp.minimum(i, nx // 2 - 1), 0, 0, 0)),
            pl.BlockSpec(matrix.shape, lambda i: (0, 0)),
        ],
        out_specs=[
            pl.BlockSpec((2, ny + 2, depth, lanes), lambda i: (i, 0, 0, 0)),
            pl.BlockSpec((1, ny + 2, depth, lanes), lambda i: (jnp.minimum(i, 1), 0, 0, 0)),
        ],
        out_shape=[
            pltpu.HBM((nx + 2, ny + 2, depth, lanes), bf16),
            jax.ShapeDtypeStruct((2, ny + 2, depth, lanes), bf16),
        ],
        scratch_shapes=[pltpu.VMEM((nx + 4, ny + 4, rows, lanes), bf16)],
        compiler_params=pltpu.CompilerParams(vmem_limit_bytes=40 * 2**20),
        cost_estimate=pl.CostEstimate(flops=9 * 10**9, bytes_accessed=12 * 2**20, transcendentals=0),
        name="conv_input_grad",
    )(in_hbm(grad_out), matrix)


def finish_call(spread, x_lo, x_hi, y_lo, y_hi, z_lo, z_hi):
    nx, ny, edge, lanes = z_lo.shape
    depth = spread.shape[2]
    width = depth - 2 * edge

    def body(spread_0, spread_1, x_lo, x_hi, y_lo, y_hi, z_lo, z_hi, result):
        step = pl.program_id(0)
        middle = slice(edge, edge + width)

        def base(x, y):
            value = (spread_0, spread_1)[x][0, y + 1, middle].astype(f32)
            if y == 0:
                value = value + y_lo[x, middle].astype(f32)
            if y == ny - 1:
                value = value + y_hi[x, middle].astype(f32)
            low = value[:edge] + z_lo[x, y].astype(f32)
            high = value[width - edge :] + z_hi[x, y].astype(f32)
            return jnp.concatenate([low, value[edge : width - edge], high], axis=0)

        def write(x, term):
            for y in range(ny):
                value = base(x, y)
                if term is not None:
                    value = value + term[y + 1, middle].astype(f32)
                result[x, y] = value.astype(bf16)

        @pl.when(step == 0)
        def _():
            write(0, x_lo)

        @pl.when(step > 0)
        def _():
            write(0, None)

        @pl.when(step == nx // 2 - 1)
        def _():
            write(1, x_hi)

        @pl.when(step < nx // 2 - 1)
        def _():
            write(1, None)

    def whole(array):
        return pl.BlockSpec(array.shape, lambda i: (0,) * array.ndim)

    def sliced(array):
        return pl.BlockSpec((2,) + array.shape[1:], lambda i: (i,) + (0,) * (array.ndim - 1))

    return pl.pallas_call(
        body,
        grid=(nx // 2,),
        in_specs=[
            pl.BlockSpec((1,) + spread.shape[1:], lambda i: (2 * i + 1, 0, 0, 0)),
            pl.BlockSpec((1,) + spread.shape[1:], lambda i: (2 * i + 2, 0, 0, 0)),
            whole(x_lo),
            whole(x_hi),
            sliced(y_lo),
            sliced(y_hi),
            sliced(z_lo),
            sliced(z_hi),
        ],
        out_specs=pl.BlockSpec((2, ny, width, lanes), lambda i: (i, 0, 0, 0)),
        out_shape=jax.ShapeDtypeStruct((nx, ny, width, lanes), bf16),
        compiler_params=pltpu.CompilerParams(vmem_limit_bytes=24 * 2**20),
        cost_estimate=pl.CostEstimate(flops=10**8, bytes_accessed=10 * 2**20, transcendentals=0),
        name="fold_faces",
    )(
        in_hbm(spread),
        in_hbm(spread),
        x_lo,
        x_hi,
        in_hbm(y_lo),
        in_hbm(y_hi),
        in_hbm(z_lo),
        in_hbm(z_hi),
    )


def feature_grad_call(weights, grad_pre_one):
    features, units = weights.shape
    samples = grad_pre_one.shape[0]
    block = features // 4

    def body(weights, grad, result):
        result[...] = lax.dot_general(
            weights[...], grad[...], (((1,), (1,)), ((), ())), preferred_element_type=f32
        ).astype(bf16)

    return pl.pallas_call(
        body,
        grid=(features // block,),
        in_specs=[
            pl.BlockSpec((block, units), lambda i: (i, 0)),
            pl.BlockSpec((samples, units), lambda i: (0, 0)),
        ],
        out_specs=pl.BlockSpec((block, samples), lambda i: (i, 0)),
        out_shape=jax.ShapeDtypeStruct((features, samples), bf16),
        compiler_params=pltpu.CompilerParams(vmem_limit_bytes=16 * 2**20),
        cost_estimate=pl.CostEstimate(flops=10**9, bytes_accessed=10 * 2**20, transcendentals=0),
        name="feature_grad",
    )(in_hbm(weights), grad_pre_one)


def exchange(array, axes):
    return lax.all_to_all(array, axes, split_axis=0, concat_axis=0, tiled=True)


def body(volume, conv_kernel, dense_one, dense_two, dense_three, targets):
    nx, ny, nz, c_in, samples = volume.shape
    c_out = conv_kernel.shape[4]
    groups_y = lax.axis_size("gy")
    groups_z = lax.axis_size("gz")
    groups = groups_y * groups_z
    devices = lax.axis_size(everyone)
    per_group = c_out // groups

    core = volume.reshape(nx, ny, nz * c_in, samples)
    x_lo, x_hi = both_ways(core[-1:], core[:1], "gx")
    first = jnp.concatenate([x_lo[:, :1], core[:, :1], x_hi[:, :1]], axis=0)
    last = jnp.concatenate([x_lo[:, -1:], core[:, -1:], x_hi[:, -1:]], axis=0)
    y_lo, y_hi = both_ways(last, first, "gy")

    def z_layer(rows):
        sides = [a[:, :, rows] for a in (y_lo, x_lo, core, x_hi, y_hi)]
        middle = jnp.concatenate(sides[1:4], axis=0)
        return jnp.concatenate([sides[0], middle, sides[4]], axis=1)

    z_lo, z_hi = both_ways(z_layer(slice(-c_in, None)), z_layer(slice(0, c_in)), "gz")
    twice = conv_kernel.reshape(-1, c_out)
    twice = jnp.concatenate([twice, twice], axis=1)
    forward_matrix, backward_matrix = banded_matrices(twice, nz, c_in)
    padded, conv_out, pooled = forward_call(
        core, x_lo[0], x_hi[0], y_lo[:, 0], y_hi[:, 0], z_lo, z_hi, forward_matrix
    )

    half_x, half_y, half_z = nx // 2, ny // 2, nz // 2
    cells = half_x * half_y * half_z
    outgoing = pooled.reshape(cells, groups, per_group, samples).transpose(1, 0, 2, 3)
    arrived = exchange(outgoing.reshape(groups, cells * per_group, samples), ("gy", "gz"))
    arrived = arrived.reshape(groups_y, groups_z, half_x, half_y, half_z, per_group, samples)
    features = arrived.transpose(2, 0, 3, 5, 1, 4, 6).reshape(-1, samples)
    weights = lax.optimization_barrier(
        dense_one.transpose(0, 1, 3, 2, 4).reshape(-1, dense_one.shape[4])
    )
    partial_one = lax.dot_general(
        features, weights, (((0,), (0,)), ((), ())), preferred_element_type=f32
    )
    rows = partial_one.shape[1] // 128
    gathered = exchange(partial_one.astype(bf16).reshape(devices, rows, 128), everyone)
    pre_one = gathered.astype(f32).sum(axis=0).reshape(1, rows * 128)
    mine = lax.axis_index(everyone)
    target = lax.dynamic_slice_in_dim(targets, mine, 1, axis=1).T
    hidden_one = smooth_leaky(pre_one)
    pre_two = jnp.dot(hidden_one, dense_two, precision=lax.Precision.HIGHEST)
    hidden_two = smooth_leaky(pre_two)
    own_prediction = jnp.dot(hidden_two, dense_three, precision=lax.Precision.HIGHEST)
    error_grad = loss_scale * (own_prediction - target)
    grad_pre_two = jnp.dot(
        error_grad, dense_three.T, precision=lax.Precision.HIGHEST
    ) * leaky_derivative(pre_two)
    own_grad = (
        jnp.dot(grad_pre_two, dense_two.T, precision=lax.Precision.HIGHEST)
        * leaky_derivative(pre_one)
    ).astype(bf16)
    copies = jnp.broadcast_to(own_grad.reshape(1, rows, 128), (devices, rows, 128))
    grad_pre_one = exchange(copies, everyone).reshape(samples, rows * 128)

    grad_features = feature_grad_call(weights, grad_pre_one)
    grad_features = grad_features.reshape(
        half_x, groups_y, half_y, per_group, groups_z, half_z, samples
    ).transpose(1, 4, 0, 2, 5, 3, 6)
    returned = exchange(grad_features.reshape(groups, cells * per_group, samples), ("gy", "gz"))
    grad_dense_one = (
        jnp.einsum("uvxyzcb,bh->xuyvzch", arrived, grad_pre_one, preferred_element_type=f32)
        / samples
    ).astype(bf16).reshape(dense_one.shape)
    grad_pooled = (
        returned.reshape(groups, cells, per_group, samples).transpose(1, 0, 2, 3)
    ).reshape(pooled.shape)

    grad_out, kernel_local = kernel_grad_call(padded, conv_out, grad_pooled, c_in)
    spread, x_faces = input_grad_call(grad_out, backward_matrix)
    from_lo, from_hi = both_ways(x_faces[1], x_faces[0], "gx")

    def added(array, first_term, last_term):
        head = (array[:1].astype(f32) + first_term.astype(f32)).astype(bf16)
        tail = (array[-1:].astype(f32) + last_term.astype(f32)).astype(bf16)
        return jnp.concatenate([head, array[1:-1], tail], axis=0)

    y_down = added(spread[1:-1, 0], from_lo[None, 0], from_hi[None, 0])
    y_up = added(spread[1:-1, -1], from_lo[None, -1], from_hi[None, -1])
    y_lo_terms, y_hi_terms = both_ways(y_up, y_down, "gy")

    def with_edges(part):
        face = spread[1:-1, 1:-1, part]
        face = added(face, from_lo[None, 1:-1, part], from_hi[None, 1:-1, part])
        head = (face[:, :1].astype(f32) + y_lo_terms[:, None, part].astype(f32)).astype(bf16)
        tail = (face[:, -1:].astype(f32) + y_hi_terms[:, None, part].astype(f32)).astype(bf16)
        return jnp.concatenate([head, face[:, 1:-1], tail], axis=1)

    z_down = with_edges(slice(0, c_in))
    z_up = with_edges(slice(-c_in, None))
    z_lo_terms, z_hi_terms = both_ways(z_up, z_down, "gz")
    grad_volume = finish_call(
        spread, from_lo, from_hi, y_lo_terms, y_hi_terms, z_lo_terms, z_hi_terms
    ).reshape(volume.shape)

    share = kernel_local.size // devices
    pieces = jnp.pad(kernel_local.reshape(devices, share), ((0, 0), (0, 512 - share)))
    pieces = exchange(pieces.reshape(devices, 4, 128), everyone)
    own_piece = (pieces.sum(axis=0) / samples).reshape(512)
    own_piece = jnp.concatenate(
        [own_piece[:share], own_prediction.reshape(-1), jnp.zeros((508 - share,), f32)]
    )
    results = exchange(
        jnp.broadcast_to(own_piece.reshape(1, 4, 128), (devices, 4, 128)), everyone
    ).reshape(devices, 512)
    grad_conv = results[:, :share].reshape(conv_kernel.shape)
    prediction = results[:, share : share + 4].T
    return (prediction, grad_dense_one, grad_conv, grad_volume)


def solution(mesh):
    return jax.shard_map(
        body,
        mesh=mesh,
        in_specs=(
            P("gx", "gy", "gz", None, None),
            P(),
            P("gx", None, None, ("gy", "gz"), None),
            P(),
            P(),
            P(),
        ),
        out_specs=(
            P(),
            P("gx", None, None, ("gy", "gz"), None),
            P(),
            P("gx", "gy", "gz", None, None),
        ),
        check_vma=False,
    )
```

```python
import jax
import jax.numpy as jnp
from jax import lax
from jax.experimental import pallas as pl
from jax.experimental.pallas import tpu as pltpu
from jax.sharding import PartitionSpec as P

loss_scale = 1024.0
leak_slope = 0.3
everyone = ("gx", "gy", "gz")
bf16 = jnp.bfloat16
f32 = jnp.float32


def in_hbm(array):
    return pltpu.with_memory_space_constraint(array, pltpu.HBM)


def neighbours(axis):
    size = lax.axis_size(axis)
    up = [(i, i + 1) for i in range(size - 1)]
    return up, [(j, i) for i, j in up]


def both_ways(toward_up, toward_down, axis):
    up, down = neighbours(axis)
    return lax.ppermute(toward_up, axis, up), lax.ppermute(toward_down, axis, down)


def smooth_leaky(values):
    return leak_slope * values + (1.0 - leak_slope) * jax.nn.softplus(values)


def leaky_derivative(values):
    return leak_slope + (1.0 - leak_slope) * jax.nn.sigmoid(values)


def banded_matrices(twice, cells, c_in):
    lanes = twice.shape[1]
    half = lanes // 2
    tap = 3 * c_in
    depth = (cells + 2) * c_in
    rows = cells * half

    def body(twice, forward, backward):
        side = lax.broadcasted_iota(jnp.int32, (tap, lanes), 1) < half
        for pair in range(cells // 2):
            for start in range(0, 9, 2):
                count = min(2, 9 - start)
                blocks = []
                for k in range(start, start + count):
                    block = twice[k * tap : (k + 1) * tap, :]
                    blocks.append(jnp.where(side, block, jnp.zeros_like(block)))
                    blocks.append(jnp.where(side, jnp.zeros_like(block), block))
                stacked = jnp.concatenate(blocks, axis=0)
                size = count * depth
                here = lax.broadcasted_iota(jnp.int32, (size, size), 0)
                from_row = lax.broadcasted_iota(jnp.int32, (size, size), 1)
                which = from_row // tap
                moved = (
                    (which // 2) * depth + (2 * pair + which % 2) * c_in + from_row - which * tap
                )
                place = jnp.where(here == moved, 1.0, 0.0).astype(bf16)
                forward[
                    pair * lanes : (pair + 1) * lanes, start * depth : (start + count) * depth
                ] = lax.dot_general(
                    stacked, place, (((0,), (1,)), ((), ())), preferred_element_type=f32
                ).astype(bf16)
                both = jnp.dot(place, stacked, preferred_element_type=f32).astype(bf16)
                for k in range(count):
                    at = (start + k) * rows + pair * lanes
                    backward[:, at : at + lanes] = both[k * depth : (k + 1) * depth]

    return pl.pallas_call(
        body,
        out_shape=[
            jax.ShapeDtypeStruct((rows, 9 * depth), bf16),
            jax.ShapeDtypeStruct((depth, 9 * rows), bf16),
        ],
        compiler_params=pltpu.CompilerParams(vmem_limit_bytes=16 * 2**20),
        cost_estimate=pl.CostEstimate(flops=10**9, bytes_accessed=2**21, transcendentals=0),
        name="banded_matrices",
    )(twice)


def forward_call(core, x_lo, x_hi, y_lo, y_hi, z_lo, z_hi, matrix):
    nx, ny, width, lanes = core.shape
    edge = z_lo.shape[2]
    depth = width + 2 * edge
    rows = matrix.shape[0]
    half = rows // 4

    def body(
        core, x_lo, x_hi, y_lo, y_hi, z_lo, z_hi, matrix, kept, conv_out, pooled, padded, sem
    ):
        step = pl.program_id(0)

        @pl.when(step == 0)
        def _():
            middle = pl.ds(edge, width)
            padded[1 : nx + 1, 1 : ny + 1, middle, :] = core[...]
            padded[0, 1 : ny + 1, middle, :] = x_lo[...]
            padded[nx + 1, 1 : ny + 1, middle, :] = x_hi[...]
            padded[:, 0, middle, :] = y_lo[...]
            padded[:, ny + 1, middle, :] = y_hi[...]
            padded[:, :, 0:edge, :] = z_lo[...]
            padded[:, :, edge + width : depth, :] = z_hi[...]
            pltpu.make_async_copy(padded, kept, sem).start()

        weights = matrix[...]
        for pair in range(ny // 2):
            y = 2 * pair
            total, factor = 0.0, 1.0
            for inner in range(2):
                x = 2 * step + inner
                patch = jnp.concatenate(
                    [
                        jnp.concatenate(
                            [padded[x + dx, y + dy], padded[x + dx, y + dy + 1]], axis=1
                        )
                        for dx in range(3)
                        for dy in range(3)
                    ],
                    axis=0,
                )
                values = jnp.dot(weights, patch, preferred_element_type=f32)
                conv_out[inner, y] = values[:, :lanes].astype(bf16)
                conv_out[inner, y + 1] = values[:, lanes:].astype(bf16)
                straight = jnp.maximum(leak_slope * values, values)
                grown = 1.0 + jnp.exp(-jnp.abs(values))
                total = total + (straight[:, :lanes] + straight[:, lanes:])
                factor = factor * (grown[:, :lanes] * grown[:, lanes:])
            for z in range(2):
                low, high = 2 * z * half, (2 * z + 1) * half
                bent = jnp.log(factor[low : low + half] * factor[high : high + half])
                mean = 0.125 * (total[low : low + half] + total[high : high + half])
                pooled[0, pair, z] = (mean + (0.125 * (1.0 - leak_slope)) * bent).astype(bf16)

        @pl.when(step == nx // 2 - 1)
        def _():
            pltpu.make_async_copy(padded, kept, sem).wait()

    def whole(array):
        return pl.BlockSpec(array.shape, lambda i: (0,) * array.ndim)

    operands = (in_hbm(core), x_lo, x_hi, y_lo, y_hi, z_lo, z_hi, matrix)
    padded_shape = (nx + 2, ny + 2, depth, lanes)
    return pl.pallas_call(
        body,
        grid=(nx // 2,),
        in_specs=[whole(a) for a in operands],
        out_specs=[
            pl.BlockSpec(memory_space=pltpu.HBM),
            pl.BlockSpec((2, ny, rows, lanes), lambda i: (i, 0, 0, 0)),
            pl.BlockSpec((1, ny // 2, 2, half, lanes), lambda i: (i, 0, 0, 0, 0)),
        ],
        out_shape=[
            pltpu.HBM(padded_shape, bf16),
            pltpu.HBM((nx, ny, rows, lanes), bf16),
            jax.ShapeDtypeStruct((nx // 2, ny // 2, 2, half, lanes), bf16),
        ],
        scratch_shapes=[
            pltpu.VMEM(padded_shape, bf16),
            pltpu.SemaphoreType.DMA,
        ],
        compiler_params=pltpu.CompilerParams(vmem_limit_bytes=40 * 2**20),
        cost_estimate=pl.CostEstimate(flops=7 * 10**9, bytes_accessed=16 * 2**20, transcendentals=0),
        name="conv_forward",
    )(*operands)


def kernel_grad_call(padded, conv_out, grad_pooled, c_in):
    nx, ny, rows, lanes = conv_out.shape
    depth = padded.shape[2]
    c_out = rows // 4

    def body(rows_0, rows_1, conv_out, grad_pooled, grad_out, result, sums):
        step = pl.program_id(0)

        @pl.when(step == 0)
        def _():
            sums[...] = jnp.zeros(sums.shape, f32)

        for x in range(2):
            for y in range(ny):
                values = conv_out[x, y].astype(f32)
                rise = (1.0 - leak_slope) / 16.0
                slope = (leak_slope / 8.0 + rise) + rise * jnp.tanh(0.5 * values)
                pieces = [grad_pooled[0, y // 2, z // 2].astype(f32) for z in range(4)]
                grad_out[x, y] = (jnp.concatenate(pieces, axis=0) * slope).astype(bf16)
        layers = [rows_0.at[0], rows_0.at[1], rows_1.at[0], rows_1.at[1]]
        right = jnp.concatenate(
            [grad_out[x, y] for x in range(2) for y in range(ny)], axis=1
        )
        for dx in range(3):
            left = jnp.concatenate(
                [
                    jnp.concatenate(
                        [layers[x + dx][y + dy] for x in range(2) for y in range(ny)], axis=1
                    )
                    for dy in range(3)
                ],
                axis=0,
            )
            sums[dx] += lax.dot_general(
                left, right, (((1,), (1,)), ((), ())), preferred_element_type=f32
            )

        @pl.when(step == nx // 2 - 1)
        def _():
            def collect(dx, carry):
                for dy in range(3):
                    for dz in range(3):
                        total = None
                        for z in range(4):
                            start = dy * depth + (z + dz) * c_in
                            piece = sums[dx, start : start + c_in, z * c_out : (z + 1) * c_out]
                            total = piece if total is None else total + piece
                        result[9 * dx + 3 * dy + dz] = total
                return carry

            lax.fori_loop(0, 3, collect, 0)

    return pl.pallas_call(
        body,
        grid=(nx // 2,),
        in_specs=[
            pl.BlockSpec((2,) + padded.shape[1:], lambda i: (i, 0, 0, 0)),
            pl.BlockSpec((2,) + padded.shape[1:], lambda i: (i + 1, 0, 0, 0)),
            pl.BlockSpec((2, ny, rows, lanes), lambda i: (i, 0, 0, 0)),
            pl.BlockSpec((1,) + grad_pooled.shape[1:], lambda i: (i, 0, 0, 0, 0)),
        ],
        out_specs=[
            pl.BlockSpec((2, ny, rows, lanes), lambda i: (i, 0, 0, 0)),
            pl.BlockSpec((27, c_in, c_out), lambda i: (0, 0, 0)),
        ],
        out_shape=[
            pltpu.HBM((nx, ny, rows, lanes), bf16),
            jax.ShapeDtypeStruct((27, c_in, c_out), f32),
        ],
        scratch_shapes=[pltpu.VMEM((3, 3 * depth, rows), f32)],
        compiler_params=pltpu.CompilerParams(vmem_limit_bytes=32 * 2**20),
        cost_estimate=pl.CostEstimate(flops=8 * 10**9, bytes_accessed=14 * 2**20, transcendentals=0),
        name="conv_kernel_grad",
    )(in_hbm(padded), in_hbm(padded), in_hbm(conv_out), grad_pooled)


def input_grad_call(grad_out, matrix):
    nx, ny, rows, lanes = grad_out.shape
    depth = matrix.shape[0]

    def body(grad_out, matrix, spread, x_first, x_last, held):
        step = pl.program_id(0)

        @pl.when(step == 0)
        def _():
            for edge in (0, nx + 2):
                held[edge : edge + 2] = jnp.zeros((2,) + held.shape[1:], bf16)
            for edge in (0, ny + 2):
                held[2 : nx + 2, edge : edge + 2] = jnp.zeros((nx, 2, rows, lanes), bf16)

        @pl.when(step < nx // 2)
        def _():
            held[pl.ds(2 * step + 2, 2), 2 : ny + 2] = grad_out[...]

        for x in range(2):
            at = 2 * step + 2 + x
            for pair in range((ny + 2) // 2):
                y = 2 * pair
                taps = [dy for dy in range(3) if y + 1 - dy >= 0 and y - dy < ny]
                values = None
                for dx in range(3):
                    patch = jnp.concatenate(
                        [
                            jnp.concatenate(
                                [held[at - dx, y + 2 - dy], held[at - dx, y + 3 - dy]], axis=1
                            )
                            for dy in taps
                        ],
                        axis=0,
                    )
                    start = (3 * dx + taps[0]) * rows
                    term = jnp.dot(
                        matrix[:, start : start + len(taps) * rows],
                        patch,
                        preferred_element_type=f32,
                    )
                    values = term if values is None else values + term
                values = values.astype(bf16)
                spread[x, y] = values[:, :lanes]
                spread[x, y + 1] = values[:, lanes:]
        x_last[...] = spread[1]

        @pl.when(step == 0)
        def _():
            x_first[...] = spread[0]

    return pl.pallas_call(
        body,
        grid=(nx // 2 + 1,),
        in_specs=[
            pl.BlockSpec((2, ny, rows, lanes), lambda i: (jnp.minimum(i, nx // 2 - 1), 0, 0, 0)),
            pl.BlockSpec(matrix.shape, lambda i: (0, 0)),
        ],
        out_specs=[
            pl.BlockSpec((2, ny + 2, depth, lanes), lambda i: (i, 0, 0, 0)),
            pl.BlockSpec((ny + 2, depth, lanes), lambda i: (0, 0, 0)),
            pl.BlockSpec((ny + 2, depth, lanes), lambda i: (0, 0, 0)),
        ],
        out_shape=[
            pltpu.HBM((nx + 2, ny + 2, depth, lanes), bf16),
            jax.ShapeDtypeStruct((ny + 2, depth, lanes), bf16),
            jax.ShapeDtypeStruct((ny + 2, depth, lanes), bf16),
        ],
        scratch_shapes=[pltpu.VMEM((nx + 4, ny + 4, rows, lanes), bf16)],
        compiler_params=pltpu.CompilerParams(vmem_limit_bytes=40 * 2**20),
        cost_estimate=pl.CostEstimate(flops=9 * 10**9, bytes_accessed=12 * 2**20, transcendentals=0),
        name="conv_input_grad",
    )(in_hbm(grad_out), matrix)


def finish_call(spread, x_lo, x_hi, y_lo, y_hi, z_lo, z_hi):
    nx, ny, edge, lanes = z_lo.shape
    depth = spread.shape[2]
    width = depth - 2 * edge

    def body(spread_0, spread_1, x_lo, x_hi, y_lo, y_hi, z_lo, z_hi, result):
        step = pl.program_id(0)
        middle = slice(edge, edge + width)

        def base(x, y):
            value = (spread_0, spread_1)[x][0, y + 1, middle].astype(f32)
            if y == 0:
                value = value + y_lo[x, middle].astype(f32)
            if y == ny - 1:
                value = value + y_hi[x, middle].astype(f32)
            low = value[:edge] + z_lo[x, y].astype(f32)
            high = value[width - edge :] + z_hi[x, y].astype(f32)
            return jnp.concatenate([low, value[edge : width - edge], high], axis=0)

        def write(x, term):
            for y in range(ny):
                value = base(x, y)
                if term is not None:
                    value = value + term[y + 1, middle].astype(f32)
                result[x, y] = value.astype(bf16)

        @pl.when(step == 0)
        def _():
            write(0, x_lo)

        @pl.when(step > 0)
        def _():
            write(0, None)

        @pl.when(step == nx // 2 - 1)
        def _():
            write(1, x_hi)

        @pl.when(step < nx // 2 - 1)
        def _():
            write(1, None)

    def whole(array):
        return pl.BlockSpec(array.shape, lambda i: (0,) * array.ndim)

    def sliced(array):
        return pl.BlockSpec((2,) + array.shape[1:], lambda i: (i,) + (0,) * (array.ndim - 1))

    return pl.pallas_call(
        body,
        grid=(nx // 2,),
        in_specs=[
            pl.BlockSpec((1,) + spread.shape[1:], lambda i: (2 * i + 1, 0, 0, 0)),
            pl.BlockSpec((1,) + spread.shape[1:], lambda i: (2 * i + 2, 0, 0, 0)),
            whole(x_lo),
            whole(x_hi),
            sliced(y_lo),
            sliced(y_hi),
            sliced(z_lo),
            sliced(z_hi),
        ],
        out_specs=pl.BlockSpec((2, ny, width, lanes), lambda i: (i, 0, 0, 0)),
        out_shape=jax.ShapeDtypeStruct((nx, ny, width, lanes), bf16),
        compiler_params=pltpu.CompilerParams(vmem_limit_bytes=24 * 2**20),
        cost_estimate=pl.CostEstimate(flops=10**8, bytes_accessed=10 * 2**20, transcendentals=0),
        name="fold_faces",
    )(
        in_hbm(spread),
        in_hbm(spread),
        x_lo,
        x_hi,
        in_hbm(y_lo),
        in_hbm(y_hi),
        z_lo,
        z_hi,
    )


def feature_grad_call(weights, grad_pre_one):
    features, units = weights.shape
    samples = grad_pre_one.shape[0]
    block = features // 4

    def body(weights, grad, result):
        result[...] = lax.dot_general(
            weights[...], grad[...], (((1,), (1,)), ((), ())), preferred_element_type=f32
        ).astype(bf16)

    return pl.pallas_call(
        body,
        grid=(features // block,),
        in_specs=[
            pl.BlockSpec((block, units), lambda i: (i, 0)),
            pl.BlockSpec((samples, units), lambda i: (0, 0)),
        ],
        out_specs=pl.BlockSpec((block, samples), lambda i: (i, 0)),
        out_shape=jax.ShapeDtypeStruct((features, samples), bf16),
        compiler_params=pltpu.CompilerParams(vmem_limit_bytes=16 * 2**20),
        cost_estimate=pl.CostEstimate(flops=10**9, bytes_accessed=10 * 2**20, transcendentals=0),
        name="feature_grad",
    )(in_hbm(weights), grad_pre_one)


def exchange(array, axes):
    return lax.all_to_all(array, axes, split_axis=0, concat_axis=0, tiled=True)


def body(volume, conv_kernel, dense_one, dense_two, dense_three, targets):
    nx, ny, nz, c_in, samples = volume.shape
    c_out = conv_kernel.shape[4]
    groups_y = lax.axis_size("gy")
    groups_z = lax.axis_size("gz")
    groups = groups_y * groups_z
    devices = lax.axis_size(everyone)
    per_group = c_out // groups

    core = volume.reshape(nx, ny, nz * c_in, samples)
    x_lo, x_hi = both_ways(core[-1:], core[:1], "gx")
    first = jnp.concatenate([x_lo[:, :1], core[:, :1], x_hi[:, :1]], axis=0)
    last = jnp.concatenate([x_lo[:, -1:], core[:, -1:], x_hi[:, -1:]], axis=0)
    y_lo, y_hi = both_ways(last, first, "gy")

    def z_layer(rows):
        sides = [a[:, :, rows] for a in (y_lo, x_lo, core, x_hi, y_hi)]
        middle = jnp.concatenate(sides[1:4], axis=0)
        return jnp.concatenate([sides[0], middle, sides[4]], axis=1)

    z_lo, z_hi = both_ways(z_layer(slice(-c_in, None)), z_layer(slice(0, c_in)), "gz")
    twice = conv_kernel.reshape(-1, c_out)
    twice = jnp.concatenate([twice, twice], axis=1)
    forward_matrix, backward_matrix = banded_matrices(twice, nz, c_in)
    padded, conv_out, pooled = forward_call(
        core, x_lo[0], x_hi[0], y_lo[:, 0], y_hi[:, 0], z_lo, z_hi, forward_matrix
    )

    half_x, half_y, half_z = nx // 2, ny // 2, nz // 2
    cells = half_x * half_y * half_z
    outgoing = pooled.reshape(cells, groups, per_group, samples).transpose(1, 0, 2, 3)
    arrived = exchange(outgoing.reshape(groups, cells * per_group, samples), ("gy", "gz"))
    arrived = arrived.reshape(groups_y, groups_z, half_x, half_y, half_z, per_group, samples)
    features = arrived.transpose(2, 0, 3, 5, 1, 4, 6).reshape(-1, samples)
    weights = lax.optimization_barrier(
        dense_one.transpose(0, 1, 3, 2, 4).reshape(-1, dense_one.shape[4])
    )
    partial_one = lax.dot_general(
        features, weights, (((0,), (0,)), ((), ())), preferred_element_type=f32
    )
    rows = partial_one.shape[1] // 128
    gathered = exchange(partial_one.astype(bf16).reshape(devices, rows, 128), everyone)
    pre_one = gathered.astype(f32).sum(axis=0).reshape(1, rows * 128)
    mine = lax.axis_index(everyone)
    target = lax.dynamic_slice_in_dim(targets, mine, 1, axis=1).T
    hidden_one = smooth_leaky(pre_one)
    pre_two = jnp.dot(hidden_one, dense_two, precision=lax.Precision.HIGHEST)
    hidden_two = smooth_leaky(pre_two)
    own_prediction = jnp.dot(hidden_two, dense_three, precision=lax.Precision.HIGHEST)
    error_grad = loss_scale * (own_prediction - target)
    grad_pre_two = jnp.dot(
        error_grad, dense_three.T, precision=lax.Precision.HIGHEST
    ) * leaky_derivative(pre_two)
    own_grad = (
        jnp.dot(grad_pre_two, dense_two.T, precision=lax.Precision.HIGHEST)
        * leaky_derivative(pre_one)
    ).astype(bf16)
    copies = jnp.broadcast_to(own_grad.reshape(1, rows, 128), (devices, rows, 128))
    grad_pre_one = exchange(copies, everyone).reshape(samples, rows * 128)

    grad_features = feature_grad_call(weights, grad_pre_one)
    grad_features = grad_features.reshape(
        half_x, groups_y, half_y, per_group, groups_z, half_z, samples
    ).transpose(1, 4, 0, 2, 5, 3, 6)
    returned = exchange(grad_features.reshape(groups, cells * per_group, samples), ("gy", "gz"))
    grad_dense_one = (
        jnp.einsum("uvxyzcb,bh->xuyvzch", arrived, grad_pre_one, preferred_element_type=f32)
        / samples
    ).astype(bf16).reshape(dense_one.shape)
    grad_pooled = (
        returned.reshape(groups, cells, per_group, samples).transpose(1, 0, 2, 3)
    ).reshape(pooled.shape)

    grad_out, kernel_local = kernel_grad_call(padded, conv_out, grad_pooled, c_in)
    spread, x_first, x_last = input_grad_call(grad_out, backward_matrix)
    from_lo, from_hi = both_ways(x_last, x_first, "gx")

    def added(array, first_term, last_term):
        head = (array[:1].astype(f32) + first_term.astype(f32)).astype(bf16)
        tail = (array[-1:].astype(f32) + last_term.astype(f32)).astype(bf16)
        return jnp.concatenate([head, array[1:-1], tail], axis=0)

    y_down = added(spread[1:-1, 0], from_lo[None, 0], from_hi[None, 0])
    y_up = added(spread[1:-1, -1], from_lo[None, -1], from_hi[None, -1])
    y_lo_terms, y_hi_terms = both_ways(y_up, y_down, "gy")

    def with_edges(part):
        face = spread[1:-1, 1:-1, part]
        face = added(face, from_lo[None, 1:-1, part], from_hi[None, 1:-1, part])
        head = (face[:, :1].astype(f32) + y_lo_terms[:, None, part].astype(f32)).astype(bf16)
        tail = (face[:, -1:].astype(f32) + y_hi_terms[:, None, part].astype(f32)).astype(bf16)
        return jnp.concatenate([head, face[:, 1:-1], tail], axis=1)

    z_down = with_edges(slice(0, c_in))
    z_up = with_edges(slice(-c_in, None))
    z_lo_terms, z_hi_terms = both_ways(z_up, z_down, "gz")
    grad_volume = finish_call(
        spread, from_lo, from_hi, y_lo_terms, y_hi_terms, z_lo_terms, z_hi_terms
    ).reshape(volume.shape)

    share = kernel_local.size // devices
    pieces = jnp.pad(kernel_local.reshape(devices, share), ((0, 0), (0, 512 - share)))
    pieces = exchange(pieces.reshape(devices, 4, 128), everyone)
    own_piece = (pieces.sum(axis=0) / samples).reshape(512)
    own_piece = jnp.concatenate(
        [own_piece[:share], own_prediction.reshape(-1), jnp.zeros((508 - share,), f32)]
    )
    results = exchange(
        jnp.broadcast_to(own_piece.reshape(1, 4, 128), (devices, 4, 128)), everyone
    ).reshape(devices, 512)
    grad_conv = results[:, :share].reshape(conv_kernel.shape)
    prediction = results[:, share : share + 4].T
    return (prediction, grad_dense_one, grad_conv, grad_volume)


def solution(mesh):
    return jax.shard_map(
        body,
        mesh=mesh,
        in_specs=(
            P("gx", "gy", "gz", None, None),
            P(),
            P("gx", None, None, ("gy", "gz"), None),
            P(),
            P(),
            P(),
        ),
        out_specs=(
            P(),
            P("gx", None, None, ("gy", "gz"), None),
            P(),
            P("gx", "gy", "gz", None, None),
        ),
        check_vma=False,
    )
```
